256 devices in a mesh: dp: 4 (over x_hi, core), expert: 64 (over y, z, x_lo).
Axes of the slice: x: 4 (x_hi: 2, x_lo: 2; x = x_hi * 2 + x_lo), y: 4, z: 8, core: 2. Of those that a mesh axis runs over, the one named last changes fastest.
Arguments:
- tokens: bfloat16 [1024, 256, 1280], P(('dp', 'expert')), may hold values from -32 to 32
- slot_keys: bfloat16 [1280, 64], replicated, may hold values from -20 to 20
- logit_scale: float32 [1], replicated, may hold values from 8 to 16
- up_weight: bfloat16 [64, 1280, 5120], P('expert', None, 'dp'), may hold values from -0.15625 to 0.15625
- up_bias: bfloat16 [64, 5120], P('expert', 'dp'), may hold values from -3 to 3
- down_weight: bfloat16 [64, 5120, 1280], P('expert', 'dp'), may hold values from -0.078125 to 0.078125
- down_bias: bfloat16 [64, 1280], replicated, may hold values from -3 to 3
Outputs:
- mixed_out: bfloat16 [1024, 256, 1280], P(('dp', 'expert'))
The draws below stay inside these ranges and needn't reach their ends.
All inputs are finite; a program needn't handle non-finite values.
Results may differ from the reference program's by a relative error of at most 0.017.
Values may be sent and summed in bfloat16 or wider, within the bound.
A program may use at most 64 MiB of HBM per device.

```python
import math
import jax
import jax.numpy as jnp
from jax import lax

D = 1280
FF = 5120
PATCHES = 256
EXPERTS = 64
IMAGES = 1024
N_DP = 4


def slot_basis(key):
    raw = jax.random.normal(jax.random.fold_in(key, 11), (D, EXPERTS), jnp.float32)
    return jnp.clip(raw, -4.0, 4.0)


def draw_slot_keys(key, part):
    basis = slot_basis(key)
    column_scale = jnp.exp(jax.random.uniform(jax.random.fold_in(key, 12), (1, EXPERTS), jnp.float32, math.log(0.5), math.log(5.0)))
    return (basis * column_scale).astype(jnp.bfloat16)


def draw_tokens(key, part):
    basis = slot_basis(key)
    rows_total = IMAGES * PATCHES
    coeffs = jnp.clip(jax.random.normal(jax.random.fold_in(key, 13), (rows_total, EXPERTS), jnp.float32), -4.0, 4.0)
    mixture = 0.2 * jnp.dot(coeffs, jnp.transpose(basis))
    noise = jnp.clip(jax.random.normal(jax.random.fold_in(key, 14), (rows_total, D), jnp.float32), -4.0, 4.0)
    row_scale = jnp.exp(jax.random.uniform(jax.random.fold_in(key, 15), (rows_total, 1), jnp.float32, math.log(0.5), math.log(5.0)))
    values = jnp.clip(row_scale * (noise + mixture), -32.0, 32.0)
    return values.reshape(IMAGES, PATCHES, D).astype(jnp.bfloat16)


def level_of(own_key, shape, pieces, smallest, largest):
    factor_of = 1.0
    for dim, blocks in pieces:
        draws = jax.random.uniform(jax.random.fold_in(jax.random.fold_in(own_key, 6), dim), (blocks,), jnp.float32, smallest / len(pieces), largest / len(pieces))
        factor_of = factor_of * jnp.repeat(jnp.exp(draws), shape[dim] // blocks).reshape((-1,) + (1,) * (len(shape) - 1 - dim))
    return factor_of


def bell_draw(key, dims, scale, bound, cuts=(), held_as=jnp.bfloat16):
    entries = scale * jax.random.normal(key, dims, jnp.float32)
    if cuts:
        entries = entries * level_of(key, dims, cuts, -0.22, 0.18)
    return jnp.clip(entries, -bound, bound).astype(held_as)


def setup_inputs(seed: int = 0) -> dict:
    key_list = jax.random.split(jax.random.key(seed), 8)
    tokens = draw_tokens(jax.random.fold_in(key_list[7], 71), 0)
    slot_keys = draw_slot_keys(jax.random.fold_in(key_list[7], 71), 0)
    logit_scale = jnp.clip(jnp.exp(jax.random.uniform(key_list[2], (1,), jnp.float32, math.log(8.0), math.log(16.0))), 8.0, 16.0)
    up_weight = bell_draw(key_list[3], (EXPERTS, D, FF), D ** -0.5, 0.15625, ((0, 64), (2, 4)))
    up_bias = bell_draw(key_list[4], (EXPERTS, FF), 0.5, 3.0, ((0, 64), (1, 4)))
    down_weight = bell_draw(key_list[5], (EXPERTS, FF, D), FF ** -0.5, 0.078125, ((0, 64), (1, 4)))
    down_bias = bell_draw(key_list[6], (EXPERTS, D), 0.5, 3.0)
    return dict(tokens=tokens, slot_keys=slot_keys, logit_scale=logit_scale, up_weight=up_weight, up_bias=up_bias, down_weight=down_weight, down_bias=down_bias)


norm_eps = 1e-06

def unit_rms(values, axis_pos):
    return values * lax.rsqrt(lax.optimization_barrier(jnp.mean(values * values, axis=axis_pos, keepdims=True)) + norm_eps)

def reference(tokens, slot_keys, logit_scale, up_weight, up_bias, down_weight, down_bias):
    normed_tok = unit_rms(tokens.astype(jnp.float32), 2).astype(jnp.bfloat16)
    normed_keys = unit_rms(slot_keys.astype(jnp.float32), 0).astype(jnp.bfloat16)
    raw_scores = jnp.einsum('ipd,dn->inp', normed_tok.astype(jnp.float32), normed_keys.astype(jnp.float32))
    logits = logit_scale[0] * raw_scores / D
    dispatch = jax.nn.softmax(logits, axis=2).astype(jnp.bfloat16)
    combine = jax.nn.softmax(logits, axis=1).astype(jnp.bfloat16)
    slot_inputs = jnp.einsum('inp,ipd->ind', dispatch.astype(jnp.float32), tokens.astype(jnp.float32)).astype(jnp.bfloat16)

    def one_expert(packed):
        slot_rows, weight_in, bias_in, weight_out = packed
        pre = jnp.dot(slot_rows, weight_in, preferred_element_type=jnp.float32) + bias_in.astype(jnp.float32)[None, :]
        hidden = jax.nn.gelu(pre, approximate=False).astype(jnp.bfloat16)
        blocks = FF // N_DP
        hidden_blocks = jnp.transpose(hidden.reshape(IMAGES, N_DP, blocks), (1, 0, 2))
        weight_blocks = weight_out.reshape(N_DP, blocks, D)
        parts = jnp.einsum('gif,gfd->gid', hidden_blocks.astype(jnp.float32), weight_blocks.astype(jnp.float32))
        parts = parts.astype(jnp.bfloat16)
        return lax.optimization_barrier(jnp.sum(parts.astype(jnp.float32), axis=0))
    summed = lax.map(one_expert, (jnp.transpose(slot_inputs, (1, 0, 2)), up_weight, up_bias, down_weight))
    expert_out = (summed + down_bias.astype(jnp.float32)[:, None, :]).astype(jnp.bfloat16)
    mixed_out = jnp.einsum('inp,nid->ipd', combine.astype(jnp.float32), expert_out.astype(jnp.float32))
    return mixed_out.astype(jnp.bfloat16)
```

```python
import functools

import jax
import jax.numpy as jnp
from jax import lax
from jax.experimental import pallas as pl
from jax.experimental.pallas import tpu as pltpu
from jax.sharding import PartitionSpec as P

norm_eps = 1e-06
MESH = pl.DeviceIdType.MESH
DC = 256
BF = jnp.bfloat16
F32 = jnp.float32


def iota(shape, dim):
    return lax.broadcasted_iota(jnp.int32, shape, dim)


def dot(a, b):
    return jnp.dot(a, b, preferred_element_type=F32)


def exchange_kernel(
    nk,
    nch,
    tok_hbm,
    keys_ref,
    scale_ref,
    up_hbm,
    upb_ref,
    down_hbm,
    downb_ref,
    comb_ref,
    out_ref,
    tok,
    disp_t,
    keyrep,
    perm,
    permt,
    wup,
    wdown,
    bup,
    bias_rows,
    slots_s,
    slots_r,
    rows,
    pre,
    hidden,
    part_s,
    part_r,
    fin,
    tok_sem,
    load_sem,
    wsend_sem,
    wrecv_sem,
    s1_sem,
    r1_sem,
    s2_sem,
    r2_sem,
    s3_sem,
    r3_sem,
    s4_sem,
    r4_sem,
):
    images, patches, width = tok.shape
    block = images * nk
    own = lax.axis_index("expert")
    dp = lax.axis_index("dp")
    k_own = lax.div(own, 2)
    parity = lax.rem(own, 2)
    flip = own + 1 - 2 * parity
    far = lax.rem(dp + 2, 4)
    core = dp + 1 - 2 * lax.rem(dp, 2)
    members = ((dp, own), (dp, flip), (far, flip), (far, own))

    def peer(step):
        k = lax.rem(k_own + step, nk)
        return k, {"dp": dp, "expert": 2 * k + parity}

    barrier = pltpu.get_barrier_semaphore()

    def greet(step, _):
        _, where = peer(step)
        pl.semaphore_signal(barrier, inc=1, device_id=where, device_id_type=MESH)
        return 0

    lax.fori_loop(1, nk, greet, 0)
    for d, e in members[1:]:
        pl.semaphore_signal(barrier, inc=1, device_id={"dp": d, "expert": e}, device_id_type=MESH)
    pl.semaphore_signal(barrier, inc=1, device_id={"dp": core, "expert": own}, device_id_type=MESH)

    tok_in = [
        pltpu.make_async_copy(tok_hbm.at[i], tok.at[i], tok_sem.at[i]) for i in range(images)
    ]
    for copy in tok_in:
        copy.start()
    up_in = pltpu.make_async_copy(up_hbm.at[0], wup.at[0], load_sem.at[0])
    down_in = pltpu.make_async_copy(down_hbm.at[0], wdown.at[0], load_sem.at[1])
    up_in.start()
    down_in.start()

    keys = keys_ref[...].astype(F32)
    keys = keys * lax.rsqrt(jnp.mean(keys * keys, axis=0, keepdims=True) + norm_eps)
    n_exp = keys.shape[1]
    spread = (lax.div(iota((n_exp, n_exp * images), 1), images) == iota((n_exp, n_exp * images), 0))
    keyrep[...] = dot(keys.astype(BF), spread.astype(BF)).astype(BF)
    row = iota(perm.shape, 0)
    col = iota(perm.shape, 1)
    rel = lax.rem(lax.div(row, block) + parity, 2)
    within = lax.rem(row, block)
    src = lax.div(within, images) * (2 * images) + rel * images + lax.rem(within, images)
    perm[...] = (src == col).astype(BF)
    row_t = iota(perm.shape, 1)
    col_t = iota(perm.shape, 0)
    rel_t = lax.rem(lax.div(row_t, block) + parity, 2)
    within_t = lax.rem(row_t, block)
    src_t = lax.div(within_t, images) * (2 * images) + rel_t * images + lax.rem(within_t, images)
    permt[...] = (src_t == col_t).astype(BF)

    n_row = 2 * k_own + lax.rem(lax.div(iota((2 * block, n_exp), 0), block) + parity, 2)
    pick = (n_row == iota((2 * block, n_exp), 1)).astype(BF)
    for c in range(nch):
        bias_rows[c] = dot(pick, downb_ref[:, c * DC : (c + 1) * DC]).astype(BF)

    scale = scale_ref[0]
    for i in range(images):
        tok_in[i].wait()
        t = tok[i]
        tf = t.astype(F32)
        factor = lax.rsqrt(jnp.mean(tf * tf, axis=1, keepdims=True) + norm_eps)
        logits = scale * (dot(t, keyrep[...]) * factor) / width
        mask = lax.rem(iota(logits.shape, 1), images) == i
        e_tok = jnp.exp(logits - jnp.max(logits, axis=0, keepdims=True))
        share = e_tok / jnp.sum(e_tok, axis=0, keepdims=True)
        share = jnp.where(mask, share, 0.0)
        disp_t[:, pl.ds(i * patches, patches)] = jnp.transpose(share).astype(BF)
        e_slot = jnp.where(mask, jnp.exp(logits - jnp.max(logits, axis=1, keepdims=True)), 0.0)
        mix = e_slot / jnp.sum(e_slot, axis=1, keepdims=True)
        comb_ref[pl.ds(i * patches, patches), :] = mix.astype(BF)

    pl.semaphore_wait(barrier, nk - 1 + 4)

    where_core = {"dp": core, "expert": own}
    sends_w = []
    for j, (src_ref, dst_ref) in enumerate(
        ((up_hbm.at[0], wup.at[1]), (down_hbm.at[0], wdown.at[1]), (upb_ref, bup))
    ):
        sends_w.append(
            pltpu.make_async_remote_copy(
                src_ref=src_ref,
                dst_ref=dst_ref,
                send_sem=wsend_sem.at[j],
                recv_sem=wrecv_sem.at[j],
                device_id=where_core,
                device_id_type=MESH,
            )
        )

    def lanes(c):
        return pl.ds(pl.multiple_of(c * DC, DC), DC)

    def send_tiles(buf, dst, c, s_sem, r_sem):
        def one(step, _):
            k, where = peer(step)
            pltpu.make_async_remote_copy(
                src_ref=buf.at[c, k],
                dst_ref=dst.at[c, k_own],
                send_sem=s_sem,
                recv_sem=r_sem.at[c],
                device_id=where,
                device_id_type=MESH,
            ).start()
            return 0

        lax.fori_loop(1, nk, one, 0)

    def dispatch(c, _):
        t = tok[:, :, lanes(c)].reshape(images * patches, DC)
        s = dot(disp_t[...], t)
        slots_s[c] = s.reshape(nk, 2 * images, DC).astype(BF)
        slots_r[c, k_own] = slots_s[c, k_own]
        send_tiles(slots_s, slots_r, c, s1_sem, r1_sem)
        return 0

    lax.fori_loop(0, nch, dispatch, 0)
    for copy in sends_w:
        copy.start()

    def to_member(src_ref, dst_ref, c, m, s_sem, r_sem):
        d, e = members[m]
        return pltpu.make_async_remote_copy(
            src_ref=src_ref,
            dst_ref=dst_ref.at[c, m],
            send_sem=s_sem,
            recv_sem=r_sem.at[c],
            device_id={"dp": d, "expert": e},
            device_id_type=MESH,
        )

    def wait_tiles(buf, c, r_sem):
        pltpu.make_async_copy(
            buf.at[c, pl.ds(0, nk - 1)], buf.at[c, pl.ds(0, nk - 1)], r_sem.at[c]
        ).wait()

    def wait_members(buf, c, r_sem):
        pltpu.make_async_copy(
            buf.at[c, pl.ds(1, 3)], buf.at[c, pl.ds(1, 3)], r_sem.at[c]
        ).wait()

    def spread_x(c, _):
        wait_tiles(slots_r, c, r1_sem)
        got = slots_r[c].reshape(2 * block, DC)
        moved = dot(perm[...], got).astype(BF)
        rows[c, 0] = moved[:block]
        rows[c, 4] = moved[block:]
        for m, piece in ((3, 0), (1, 4), (2, 4)):
            to_member(rows.at[c, piece], rows, c, m, s2_sem, r2_sem).start()
        return 0

    def up(c, first):
        wait_members(rows, c, r2_sem)
        x = rows[c, pl.ds(0, 4)].reshape(4 * block, DC)

        def one(j, _):
            half = lax.div(j, nch)
            cols = lanes(lax.rem(j, nch))
            part = dot(x, wup[half, lanes(c), cols])
            pre[j] = part if first else pre[j] + part
            return 0

        lax.fori_loop(0, 2 * nch, one, 0)
        return 0

    spread_x(0, 0)
    up_in.wait()
    sends_w[0].wait_recv()
    spread_x(1, 0)
    up(0, True)

    def spread_and_up(c, _):
        spread_x(c, 0)
        up(c - 1, False)
        return 0

    lax.fori_loop(2, nch, spread_and_up, 0)
    up(nch - 1, False)

    sends_w[2].wait_recv()

    def activate(half, bias_ref):
        def one(j, _):
            v = pre[half * nch + j] + bias_ref[:, lanes(j)].astype(F32)
            h = 0.5 * v * (1.0 + lax.erf(v * (2.0**-0.5)))
            hidden[:, lanes(half * nch + j)] = h.astype(BF)
            return 0

        lax.fori_loop(0, nch, one, 0)

    activate(0, upb_ref)
    activate(1, bup)
    down_in.wait()
    sends_w[1].wait_recv()

    def down(c, _):
        p = dot(hidden[:, pl.ds(0, width)], wdown[0, :, lanes(c)])
        p = p + dot(hidden[:, pl.ds(width, width)], wdown[1, :, lanes(c)])
        part_s[c] = p.astype(BF).reshape(4, block, DC)
        for m in (3, 1, 2):
            to_member(part_s.at[c, m], part_r, c, m, s3_sem, r3_sem).start()
        return 0

    lax.fori_loop(0, nch, down, 0)

    def finish(c, _):
        wait_members(part_r, c, r3_sem)
        mine = part_s[c, 0].astype(F32) + part_r[c, 3].astype(F32)
        other = part_r[c, 1].astype(F32) + part_r[c, 2].astype(F32)
        total = jnp.concatenate([mine, other], axis=0) + bias_rows[c].astype(F32)
        moved = dot(permt[...], total.astype(BF))
        fin[c] = moved.reshape(nk, 2 * images, DC).astype(BF)
        out_ref[c, k_own] = fin[c, k_own]
        send_tiles(fin, out_ref, c, s4_sem, r4_sem)
        return 0

    lax.fori_loop(0, nch, finish, 0)

    def arrive(c, _):
        wait_tiles(out_ref, c, r4_sem)
        return 0

    lax.fori_loop(0, nch, arrive, 0)

    def drain(buf, first, count, sem):
        view = buf.at[:, pl.ds(first, count)]
        pltpu.make_async_copy(view, view, sem).wait()

    for copy in sends_w:
        copy.wait_send()
    drain(slots_s, 0, nk - 1, s1_sem)
    drain(rows, 1, 3, s2_sem)
    drain(part_s, 1, 3, s3_sem)
    drain(fin, 0, nk - 1, s4_sem)


def mix_kernel(nch, comb_ref, got_ref, out_ref):
    n = comb_ref.shape[1]
    for c in range(nch):
        r = got_ref[c].reshape(n, DC)
        out_ref[0, :, c * DC : (c + 1) * DC] = dot(comb_ref[...], r).astype(BF)


def body(tokens, slot_keys, logit_scale, up_weight, up_bias, down_weight, down_bias):
    images, patches, width = tokens.shape
    nk = lax.axis_size("expert") // 2
    nch = width // DC
    n_exp = 2 * nk
    cols = n_exp * images
    block = images * nk
    hid = up_weight.shape[2]
    dma = pltpu.SemaphoreType.DMA
    vmem = pl.BlockSpec(memory_space=pltpu.VMEM)
    anym = pl.BlockSpec(memory_space=pl.ANY)
    comb, got = pl.pallas_call(
        functools.partial(exchange_kernel, nk, nch),
        out_shape=(
            jax.ShapeDtypeStruct((images * patches, cols), BF),
            jax.ShapeDtypeStruct((nch, nk, 2 * images, DC), BF),
        ),
        in_specs=[anym, vmem, pl.BlockSpec(memory_space=pltpu.SMEM), anym, vmem, anym, vmem],
        out_specs=(vmem, vmem),
        scratch_shapes=[
            pltpu.VMEM((images, patches, width), BF),
            pltpu.VMEM((cols, images * patches), BF),
            pltpu.VMEM((width, cols), BF),
            pltpu.VMEM((2 * block, 2 * block), BF),
            pltpu.VMEM((2 * block, 2 * block), BF),
            pltpu.VMEM((2, width, hid), BF),
            pltpu.VMEM((2, hid, width), BF),
            pltpu.VMEM((1, hid), BF),
            pltpu.VMEM((nch, 2 * block, DC), BF),
            pltpu.VMEM((nch, nk, 2 * images, DC), BF),
            pltpu.VMEM((nch, nk, 2 * images, DC), BF),
            pltpu.VMEM((nch, 5, block, DC), BF),
            pltpu.VMEM((2 * nch, 4 * block, DC), F32),
            pltpu.VMEM((4 * block, 2 * hid), BF),
            pltpu.VMEM((nch, 4, block, DC), BF),
            pltpu.VMEM((nch, 4, block, DC), BF),
            pltpu.VMEM((nch, nk, 2 * images, DC), BF),
            dma((images,)),
            dma((2,)),
            dma((3,)),
            dma((3,)),
            dma,
            dma((nch,)),
            dma,
            dma((nch,)),
            dma,
            dma((nch,)),
            dma,
            dma((nch,)),
        ],
        compiler_params=pltpu.CompilerParams(
            collective_id=0, has_side_effects=True, vmem_limit_bytes=60 * 1024 * 1024
        ),
        name="exchange",
    )(tokens, slot_keys, logit_scale, up_weight, up_bias, down_weight, down_bias)
    return pl.pallas_call(
        functools.partial(mix_kernel, nch),
        grid=(images,),
        out_shape=jax.ShapeDtypeStruct(tokens.shape, BF),
        in_specs=[
            pl.BlockSpec((patches, cols), lambda i: (i, 0)),
            pl.BlockSpec((nch, nk, 2 * images, DC), lambda i: (0, 0, 0, 0)),
        ],
        out_specs=pl.BlockSpec((1, patches, width), lambda i: (i, 0, 0)),
        name="mix",
    )(comb, got)


def solution(mesh):
    return jax.shard_map(
        body,
        mesh=mesh,
        in_specs=(
            P(("dp", "expert"), None, None),
            P(),
            P(),
            P("expert", None, "dp"),
            P("expert", "dp"),
            P("expert", "dp", None),
            P(),
        ),
        out_specs=P(("dp", "expert"), None, None),
        check_vma=False,
    )
```

```python
import functools

import jax
import jax.numpy as jnp
from jax import lax
from jax.experimental import pallas as pl
from jax.experimental.pallas import tpu as pltpu
from jax.sharding import PartitionSpec as P

norm_eps = 1e-06
MESH = pl.DeviceIdType.MESH
DC = 256
BF = jnp.bfloat16
F32 = jnp.float32


def iota(shape, dim):
    return lax.broadcasted_iota(jnp.int32, shape, dim)


def dot(a, b):
    return jnp.dot(a, b, preferred_element_type=F32)


def exchange_kernel(
    nk,
    nch,
    tok_hbm,
    keys_hbm,
    scale_hbm,
    up_hbm,
    upb_hbm,
    down_hbm,
    downb_hbm,
    out_ref,
    tok,
    keys_ref,
    scale_ref,
    upb_ref,
    downb_ref,
    disp_t,
    keyrep,
    scores,
    perm,
    permt,
    wup,
    wdown,
    bup,
    bias_rows,
    slots_s,
    slots_r,
    rows,
    pre,
    hidden,
    part_s,
    part_r,
    fin,
    comb,
    got,
    tok_sem,
    load_sem,
    wsend_sem,
    wrecv_sem,
    s1_sem,
    r1_sem,
    s2_sem,
    r2_sem,
    s3_sem,
    r3_sem,
    s4_sem,
    r4_sem,
):
    images, patches, width = tok.shape
    block = images * nk
    own = lax.axis_index("expert")
    dp = lax.axis_index("dp")
    k_own = lax.div(own, 2)
    parity = lax.rem(own, 2)
    flip = own + 1 - 2 * parity
    far = lax.rem(dp + 2, 4)
    core = dp + 1 - 2 * lax.rem(dp, 2)
    members = ((dp, own), (dp, flip), (far, flip), (far, own))

    def peer(step):
        k = lax.rem(k_own + step, nk)
        return k, {"dp": dp, "expert": 2 * k + parity}

    tok_in = [
        pltpu.make_async_copy(tok_hbm.at[i], tok.at[i], tok_sem.at[i]) for i in range(images)
    ]
    keys_in = pltpu.make_async_copy(keys_hbm, keys_ref, load_sem.at[2])
    scale_in = pltpu.make_async_copy(scale_hbm, scale_ref, load_sem.at[3])
    upb_in = pltpu.make_async_copy(upb_hbm, upb_ref, load_sem.at[4])
    downb_in = pltpu.make_async_copy(downb_hbm, downb_ref, load_sem.at[5])
    for copy in (keys_in, scale_in, *tok_in, upb_in, downb_in):
        copy.start()
    up_in = pltpu.make_async_copy(up_hbm.at[0], wup.at[0], load_sem.at[0])
    down_in = pltpu.make_async_copy(down_hbm.at[0], wdown.at[0], load_sem.at[1])
    up_in.start()
    down_in.start()

    barrier = pltpu.get_barrier_semaphore()

    def greet(step, _):
        _, where = peer(step)
        pl.semaphore_signal(barrier, inc=1, device_id=where, device_id_type=MESH)
        return 0

    lax.fori_loop(1, nk, greet, 0)
    for d, e in members[1:]:
        pl.semaphore_signal(barrier, inc=1, device_id={"dp": d, "expert": e}, device_id_type=MESH)
    pl.semaphore_signal(barrier, inc=1, device_id={"dp": core, "expert": own}, device_id_type=MESH)

    keys_in.wait()
    keys = keys_ref[...].astype(F32)
    keys = keys * lax.rsqrt(jnp.mean(keys * keys, axis=1, keepdims=True) + norm_eps)
    n_exp = keys.shape[0]
    spread = lax.div(iota((n_exp * images, n_exp), 0), images) == iota((n_exp * images, n_exp), 1)
    keyrep[...] = jnp.transpose(dot(spread.astype(BF), keys.astype(BF))).astype(BF)

    scale_in.wait()
    scale = scale_ref[0]
    for i in range(images):
        tok_in[i].wait()
        t = tok[i]
        tf = t.astype(F32)
        factor = lax.rsqrt(jnp.mean(tf * tf, axis=1, keepdims=True) + norm_eps)
        logits = scale * (dot(t, keyrep[...]) * factor) / width
        scores[pl.ds(i * patches, patches), :] = logits
        mask = lax.rem(iota(logits.shape, 1), images) == i
        e_tok = jnp.exp(logits - jnp.max(logits, axis=0, keepdims=True))
        share = e_tok / jnp.sum(e_tok, axis=0, keepdims=True)
        share = jnp.where(mask, share, 0.0)
        disp_t[:, pl.ds(i * patches, patches)] = jnp.transpose(share).astype(BF)

    pl.semaphore_wait(barrier, nk - 1 + 4)

    where_core = {"dp": core, "expert": own}
    sends_w = []
    for j, (src_ref, dst_ref) in enumerate(
        ((up_hbm.at[0], wup.at[1]), (down_hbm.at[0], wdown.at[1]), (upb_hbm, bup))
    ):
        sends_w.append(
            pltpu.make_async_remote_copy(
                src_ref=src_ref,
                dst_ref=dst_ref,
                send_sem=wsend_sem.at[j],
                recv_sem=wrecv_sem.at[j],
                device_id=where_core,
                device_id_type=MESH,
            )
        )

    def lanes(c):
        return pl.ds(pl.multiple_of(c * DC, DC), DC)

    def send_tiles(buf, dst, c, s_sem, r_sem):
        def one(step, _):
            k, where = peer(step)
            pltpu.make_async_remote_copy(
                src_ref=buf.at[c, k],
                dst_ref=dst.at[c, k_own],
                send_sem=s_sem,
                recv_sem=r_sem.at[c],
                device_id=where,
                device_id_type=MESH,
            ).start()
            return 0

        lax.fori_loop(1, nk, one, 0)

    def dispatch(c, _):
        t = tok[:, :, lanes(c)].reshape(images * patches, DC)
        s = dot(disp_t[...], t)
        slots_s[c] = s.reshape(nk, 2 * images, DC).astype(BF)
        slots_r[c, k_own] = slots_s[c, k_own]
        send_tiles(slots_s, slots_r, c, s1_sem, r1_sem)
        return 0

    for copy in sends_w:
        copy.start()
    lax.fori_loop(0, nch, dispatch, 0)

    row = iota(perm.shape, 0)
    col = iota(perm.shape, 1)
    rel = lax.rem(lax.div(row, block) + parity, 2)
    within = lax.rem(row, block)
    src = lax.div(within, images) * (2 * images) + rel * images + lax.rem(within, images)
    perm[...] = (src == col).astype(BF)
    row_t = iota(perm.shape, 1)
    col_t = iota(perm.shape, 0)
    rel_t = lax.rem(lax.div(row_t, block) + parity, 2)
    within_t = lax.rem(row_t, block)
    src_t = lax.div(within_t, images) * (2 * images) + rel_t * images + lax.rem(within_t, images)
    permt[...] = (src_t == col_t).astype(BF)

    downb_in.wait()
    n_row = 2 * k_own + lax.rem(lax.div(iota((2 * block, n_exp), 0), block) + parity, 2)
    pick = (n_row == iota((2 * block, n_exp), 1)).astype(BF)
    for c in range(nch):
        bias_rows[c] = dot(pick, downb_ref[:, c * DC : (c + 1) * DC]).astype(BF)

    def mix_weights(i, _):
        tokens_of = pl.ds(pl.multiple_of(i * patches, patches), patches)
        logits = scores[tokens_of, :]
        mask = lax.rem(iota(logits.shape, 1), images) == i
        e_slot = jnp.where(mask, jnp.exp(logits - jnp.max(logits, axis=1, keepdims=True)), 0.0)
        mix = e_slot / jnp.sum(e_slot, axis=1, keepdims=True)
        comb[tokens_of, :] = mix.astype(BF)
        return 0

    lax.fori_loop(0, images, mix_weights, 0)

    def to_member(src_ref, dst_ref, c, m, s_sem, r_sem):
        d, e = members[m]
        return pltpu.make_async_remote_copy(
            src_ref=src_ref,
            dst_ref=dst_ref.at[c, m],
            send_sem=s_sem,
            recv_sem=r_sem.at[c],
            device_id={"dp": d, "expert": e},
            device_id_type=MESH,
        )

    def wait_tiles(buf, c, r_sem):
        pltpu.make_async_copy(
            buf.at[c, pl.ds(0, nk - 1)], buf.at[c, pl.ds(0, nk - 1)], r_sem.at[c]
        ).wait()

    def wait_members(buf, c, r_sem):
        pltpu.make_async_copy(
            buf.at[c, pl.ds(1, 3)], buf.at[c, pl.ds(1, 3)], r_sem.at[c]
        ).wait()

    def spread_x(c, _):
        wait_tiles(slots_r, c, r1_sem)
        got = slots_r[c].reshape(2 * block, DC)
        moved = dot(perm[...], got).astype(BF)
        rows[c, 0] = moved[:block]
        rows[c, 4] = moved[block:]
        for m, piece in ((3, 0), (1, 4), (2, 4)):
            to_member(rows.at[c, piece], rows, c, m, s2_sem, r2_sem).start()
        return 0

    def up(c, first):
        wait_members(rows, c, r2_sem)
        x = rows[c, pl.ds(0, 4)].reshape(4 * block, DC)

        for j in range(2 * nch):
            half, at = divmod(j, nch)
            part = dot(x, wup[half, lanes(c), at * DC : (at + 1) * DC])
            pre[j] = part if first else pre[j] + part
        return 0

    spread_x(0, 0)
    up_in.wait()
    sends_w[0].wait_recv()
    spread_x(1, 0)
    up(0, True)

    def spread_and_up(c, _):
        spread_x(c, 0)
        up(c - 1, False)
        return 0

    lax.fori_loop(2, nch, spread_and_up, 0)
    up(nch - 1, False)

    sends_w[2].wait_recv()

    def activate(half, bias_ref):
        def one(j, _):
            v = pre[half * nch + j] + bias_ref[:, lanes(j)].astype(F32)
            h = 0.5 * v * (1.0 + lax.erf(v * (2.0**-0.5)))
            hidden[:, lanes(half * nch + j)] = h.astype(BF)
            return 0

        lax.fori_loop(0, nch, one, 0)

    upb_in.wait()
    activate(0, upb_ref)
    activate(1, bup)
    down_in.wait()
    sends_w[1].wait_recv()

    def down(c, _):
        p = dot(hidden[:, pl.ds(0, width)], wdown[0, :, lanes(c)])
        p = p + dot(hidden[:, pl.ds(width, width)], wdown[1, :, lanes(c)])
        part_s[c] = p.astype(BF).reshape(4, block, DC)
        for m in (3, 1, 2):
            to_member(part_s.at[c, m], part_r, c, m, s3_sem, r3_sem).start()
        return 0

    lax.fori_loop(0, nch, down, 0)

    def finish(c, _):
        wait_members(part_r, c, r3_sem)
        mine = part_s[c, 0].astype(F32) + part_r[c, 3].astype(F32)
        other = part_r[c, 1].astype(F32) + part_r[c, 2].astype(F32)
        total = jnp.concatenate([mine, other], axis=0) + bias_rows[c].astype(F32)
        moved = dot(permt[...], total.astype(BF))
        fin[c] = moved.reshape(nk, 2 * images, DC).astype(BF)
        got[c, k_own] = fin[c, k_own]
        send_tiles(fin, got, c, s4_sem, r4_sem)
        return 0

    lax.fori_loop(0, nch, finish, 0)

    def arrive(c, _):
        wait_tiles(got, c, r4_sem)
        back = got[c].reshape(2 * block, DC)
        for i in range(images):
            mixed = dot(comb[pl.ds(i * patches, patches), :], back)
            out_ref[i, :, lanes(c)] = mixed.astype(BF)
        return 0

    lax.fori_loop(0, nch, arrive, 0)

    def drain(buf, first, count, sem):
        view = buf.at[:, pl.ds(first, count)]
        pltpu.make_async_copy(view, view, sem).wait()

    for copy in sends_w:
        copy.wait_send()
    drain(slots_s, 0, nk - 1, s1_sem)
    drain(rows, 1, 3, s2_sem)
    drain(part_s, 1, 3, s3_sem)
    drain(fin, 0, nk - 1, s4_sem)


def body(tokens, slot_keys, logit_scale, up_weight, up_bias, down_weight, down_bias):
    images, patches, width = tokens.shape
    nk = lax.axis_size("expert") // 2
    nch = width // DC
    n_exp = 2 * nk
    cols = n_exp * images
    block = images * nk
    hid = up_weight.shape[2]
    dma = pltpu.SemaphoreType.DMA
    vmem = pl.BlockSpec(memory_space=pltpu.VMEM)
    hbm = pl.BlockSpec(memory_space=pltpu.HBM)
    return pl.pallas_call(
        functools.partial(exchange_kernel, nk, nch),
        out_shape=pltpu.VMEM(tokens.shape, BF),
        in_specs=[hbm] * 7,
        out_specs=vmem,
        scratch_shapes=[
            pltpu.VMEM((images, patches, width), BF),
            pltpu.VMEM((n_exp, width), BF),
            pltpu.SMEM((1,), F32),
            pltpu.VMEM((1, hid), BF),
            pltpu.VMEM((n_exp, width), BF),
            pltpu.VMEM((cols, images * patches), BF),
            pltpu.VMEM((width, cols), BF),
            pltpu.VMEM((images * patches, cols), F32),
            pltpu.VMEM((2 * block, 2 * block), BF),
            pltpu.VMEM((2 * block, 2 * block), BF),
            pltpu.VMEM((2, width, hid), BF),
            pltpu.VMEM((2, hid, width), BF),
            pltpu.VMEM((1, hid), BF),
            pltpu.VMEM((nch, 2 * block, DC), BF),
            pltpu.VMEM((nch, nk, 2 * images, DC), BF),
            pltpu.VMEM((nch, nk, 2 * images, DC), BF),
            pltpu.VMEM((nch, 5, block, DC), BF),
            pltpu.VMEM((2 * nch, 4 * block, DC), F32),
            pltpu.VMEM((4 * block, 2 * hid), BF),
            pltpu.VMEM((nch, 4, block, DC), BF),
            pltpu.VMEM((nch, 4, block, DC), BF),
            pltpu.VMEM((nch, nk, 2 * images, DC), BF),
            pltpu.VMEM((images * patches, cols), BF),
            pltpu.VMEM((nch, nk, 2 * images, DC), BF),
            dma((images,)),
            dma((6,)),
            dma((3,)),
            dma((3,)),
            dma,
            dma((nch,)),
            dma,
            dma((nch,)),
            dma,
            dma((nch,)),
            dma,
            dma((nch,)),
        ],
        compiler_params=pltpu.CompilerParams(
            collective_id=0, has_side_effects=True, vmem_limit_bytes=58 * 1024 * 1024
        ),
        name="exchange",
    )(tokens, slot_keys.T, logit_scale, up_weight, up_bias, down_weight, down_bias)


def solution(mesh):
    return jax.shard_map(
        body,
        mesh=mesh,
        in_specs=(
            P(("dp", "expert"), None, None),
            P(),
            P(),
            P("expert", None, "dp"),
            P("expert", "dp"),
            P("expert", "dp", None),
            P(),
        ),
        out_specs=P(("dp", "expert"), None, None),
        check_vma=False,
    )
```

```python
import functools

import jax
import jax.numpy as jnp
from jax import lax
from jax.experimental import pallas as pl
from jax.experimental.pallas import tpu as pltpu
from jax.sharding import PartitionSpec as P

norm_eps = 1e-06
MESH = pl.DeviceIdType.MESH
LN = 128
DC = 2 * LN
HALVES = 2
BF = jnp.bfloat16
F32 = jnp.float32


def iota(shape, dim):
    return lax.broadcasted_iota(jnp.int32, shape, dim)


def dot(a, b):
    return jnp.dot(a, b, preferred_element_type=F32)


def exchange_kernel(
    nk,
    nch,
    tok_hbm,
    keys_hbm,
    scale_hbm,
    up_hbm,
    upb_hbm,
    down_hbm,
    downb_hbm,
    out_ref,
    tok,
    keys_ref,
    scale_ref,
    upb_ref,
    downb_ref,
    disp_t,
    keyrep,
    scores,
    perm,
    permt,
    wup,
    wdown,
    bup,
    bias_rows,
    slots_s,
    slots_r,
    rows,
    pre,
    hidden,
    part_s,
    part_r,
    fin,
    comb,
    got,
    tok_sem,
    load_sem,
    wsend_sem,
    wrecv_sem,
    s1_sem,
    r1_sem,
    s2_sem,
    r2_sem,
    s3_sem,
    r3_sem,
    s4_sem,
    r4_sem,
):
    images, patches, width = tok.shape
    ih = images // HALVES
    tile = 4 * ih
    sub = nk * ih
    block = 2 * sub
    n_exp = keys_ref.shape[0]
    units = HALVES * nch
    own = lax.axis_index("expert")
    dp = lax.axis_index("dp")
    k_own = lax.div(own, 2)
    parity = lax.rem(own, 2)
    flip = own + 1 - 2 * parity
    far = lax.rem(dp + 2, 4)
    core = dp + 1 - 2 * lax.rem(dp, 2)
    members = ((dp, own), (dp, flip), (far, flip), (far, own))

    def peer(step):
        k = lax.rem(k_own + step, nk)
        return k, {"dp": dp, "expert": 2 * k + parity}

    tok_in = [
        pltpu.make_async_copy(tok_hbm.at[i], tok.at[i], tok_sem.at[i]) for i in range(images)
    ]
    keys_in = pltpu.make_async_copy(keys_hbm, keys_ref, load_sem.at[2])
    scale_in = pltpu.make_async_copy(scale_hbm, scale_ref, load_sem.at[3])
    upb_in = pltpu.make_async_copy(upb_hbm, upb_ref, load_sem.at[4])
    downb_in = pltpu.make_async_copy(downb_hbm, downb_ref, load_sem.at[5])
    for copy in (keys_in, scale_in, *tok_in, upb_in, downb_in):
        copy.start()
    up_in = pltpu.make_async_copy(up_hbm.at[0], wup.at[0], load_sem.at[0])
    down_in = pltpu.make_async_copy(down_hbm.at[0], wdown.at[0], load_sem.at[1])
    up_in.start()
    down_in.start()

    barrier = pltpu.get_barrier_semaphore()

    def greet(step, _):
        _, where = peer(step)
        pl.semaphore_signal(barrier, inc=1, device_id=where, device_id_type=MESH)
        return 0

    for step in range(1, nk):
        greet(step, 0)
    for d, e in members[1:]:
        pl.semaphore_signal(barrier, inc=1, device_id={"dp": d, "expert": e}, device_id_type=MESH)
    pl.semaphore_signal(barrier, inc=1, device_id={"dp": core, "expert": own}, device_id_type=MESH)

    keys_in.wait()
    keys = keys_ref[...].astype(F32)
    keys = keys * lax.rsqrt(jnp.mean(keys * keys, axis=1, keepdims=True) + norm_eps)
    col = iota((nk * tile, n_exp), 0)
    col = 2 * lax.div(col, tile) + lax.rem(lax.div(col, ih), 2)
    spread = (col == iota((nk * tile, n_exp), 1)).astype(BF)
    keyrep[...] = jnp.transpose(dot(spread, keys.astype(BF))).astype(BF)

    def place_mask(shape, dim, i, cc):
        at = iota(shape, dim)
        return (lax.rem(at, ih) == i) & (lax.rem(lax.div(at, 2 * ih), 2) == cc)

    scale_in.wait()
    scale = scale_ref[0]

    def soften(images_of):
        for i in images_of:
            tok_in[i].wait()
            t = tok[i]
            tf = t.astype(F32)
            factor = lax.rsqrt(jnp.mean(tf * tf, axis=1, keepdims=True) + norm_eps)
            logits = scale * (dot(t, keyrep[...]) * factor) / width
            scores[pl.ds(i * patches, patches), :] = logits
            e_tok = jnp.exp(logits - jnp.max(logits, axis=0, keepdims=True))
            share = jnp.transpose(e_tok / jnp.sum(e_tok, axis=0, keepdims=True))
            half, at = divmod(i, ih)
            for cc in range(2):
                kept = jnp.where(place_mask(share.shape, 0, at, cc), share, 0.0)
                disp_t[half, cc, :, pl.ds(at * patches, patches)] = kept.astype(BF)

    soften(range(ih))

    pl.semaphore_wait(barrier, nk - 1 + 4)

    where_core = {"dp": core, "expert": own}
    sends_w = []
    for j, (src_ref, dst_ref) in enumerate(
        ((up_hbm.at[0], wup.at[1]), (down_hbm.at[0], wdown.at[1]), (upb_hbm, bup))
    ):
        sends_w.append(
            pltpu.make_async_remote_copy(
                src_ref=src_ref,
                dst_ref=dst_ref,
                send_sem=wsend_sem.at[j],
                recv_sem=wrecv_sem.at[j],
                device_id=where_core,
                device_id_type=MESH,
            )
        )

    def lanes(c):
        return pl.ds(pl.multiple_of(c * DC, DC), DC)

    def lane_tile(c, cc):
        return pl.ds(pl.multiple_of(c * DC + cc * LN, LN), LN)

    def of(u):
        half = lax.div(u, nch)
        return half, u - half * nch

    def send_tiles(buf, dst, u, s_sem, r_sem):
        def one(step, _):
            k, where = peer(step)
            pltpu.make_async_remote_copy(
                src_ref=buf.at[u, k],
                dst_ref=dst.at[u, k_own],
                send_sem=s_sem,
                recv_sem=r_sem.at[u],
                device_id=where,
                device_id_type=MESH,
            ).start()
            return 0

        for step in range(1, nk):
            one(step, 0)

    def dispatch(u):
        half, c = of(u)
        ts = tok[pl.ds(half * ih, ih), :, lanes(c)].reshape(ih * patches, DC)
        s = dot(disp_t[half, 0], ts[:, :LN]) + dot(disp_t[half, 1], ts[:, LN:])
        slots_s[u] = s.reshape(nk, tile, LN).astype(BF)
        slots_r[u, k_own] = slots_s[u, k_own]
        send_tiles(slots_s, slots_r, u, s1_sem, r1_sem)

    def to_member(src_ref, dst_ref, u, m, s_sem, r_sem):
        d, e = members[m]
        return pltpu.make_async_remote_copy(
            src_ref=src_ref,
            dst_ref=dst_ref.at[u, m],
            send_sem=s_sem,
            recv_sem=r_sem.at[u],
            device_id={"dp": d, "expert": e},
            device_id_type=MESH,
        )

    def wait_tiles(buf, u, r_sem):
        view = buf.at[u, pl.ds(0, nk - 1)]
        pltpu.make_async_copy(view, view, r_sem.at[u]).wait()

    def wait_members(buf, u, r_sem):
        view = buf.at[u, pl.ds(1, 3)]
        pltpu.make_async_copy(view, view, r_sem.at[u]).wait()

    def spread_x(u):
        wait_tiles(slots_r, u, r1_sem)
        moved = dot(perm[...], slots_r[u].reshape(2 * block, LN)).astype(BF)
        rows[u, 0] = moved[:block]
        rows[u, 4] = moved[block:]
        for m, piece in ((3, 0), (1, 4), (2, 4)):
            to_member(rows.at[u, piece], rows, u, m, s2_sem, r2_sem).start()

    def up(u):
        half, c = of(u)
        wait_members(rows, u, r2_sem)
        x = jnp.concatenate(
            [rows[u, pl.ds(0, 4), pl.ds(0, sub)], rows[u, pl.ds(0, 4), pl.ds(sub, sub)]], axis=2
        ).reshape(4 * sub, DC)
        for j in range(2 * nch):
            which, at = divmod(j, nch)
            pre[half, j] += dot(x, wup[which, lanes(c), at * DC : (at + 1) * DC])

    def activate(half):
        for which, bias_ref in ((0, upb_ref), (1, bup)):

            def one(j, _, which=which, bias_ref=bias_ref):
                v = pre[half, which * nch + j] + bias_ref[:, lanes(j)].astype(F32)
                h = 0.5 * v * (1.0 + lax.erf(v * (2.0**-0.5)))
                hidden[half, :, lanes(which * nch + j)] = h.astype(BF)
                return 0

            lax.fori_loop(0, nch, one, 0)

    def down(u):
        half, c = of(u)
        p = dot(hidden[half, :, pl.ds(0, width)], wdown[0, :, lanes(c)])
        p = p + dot(hidden[half, :, pl.ds(width, width)], wdown[1, :, lanes(c)])
        p = p.astype(BF)
        part_s[u, :, pl.ds(0, sub)] = p[:, :LN].reshape(4, sub, LN)
        part_s[u, :, pl.ds(sub, sub)] = p[:, LN:].reshape(4, sub, LN)
        for m in (3, 1, 2):
            to_member(part_s.at[u, m], part_r, u, m, s3_sem, r3_sem).start()

    def finish(u):
        half, c = of(u)
        wait_members(part_r, u, r3_sem)
        mine = part_s[u, 0].astype(F32) + part_r[u, 3].astype(F32)
        other = part_r[u, 1].astype(F32) + part_r[u, 2].astype(F32)
        total = jnp.concatenate([mine, other], axis=0) + bias_rows[c].astype(F32)
        moved = dot(permt[...], total.astype(BF))
        fin[u] = moved.reshape(nk, tile, LN).astype(BF)
        got[u, k_own] = fin[u, k_own]
        send_tiles(fin, got, u, s4_sem, r4_sem)

    def mix(u):
        half, c = of(u)
        wait_tiles(got, u, r4_sem)
        back = got[u].reshape(2 * block, LN)
        for at in range(ih):
            for cc in range(2):
                mixed = dot(comb[half, cc, pl.ds(at * patches, patches), :], back)
                out_ref[half * ih + at, :, lane_tile(c, cc)] = mixed.astype(BF)

    def mix_weights(i, _):
        logits = scores[pl.ds(pl.multiple_of(i * patches, patches), patches), :]
        half = lax.div(i, ih)
        at = lax.rem(i, ih)
        masks = [place_mask(logits.shape, 1, at, cc) for cc in range(2)]
        e_slot = jnp.exp(logits - jnp.max(logits, axis=1, keepdims=True))
        total = jnp.sum(jnp.where(masks[0], e_slot, 0.0), axis=1, keepdims=True)
        share = e_slot / total
        for cc in range(2):
            kept = jnp.where(masks[cc], share, 0.0)
            comb[half, cc, pl.ds(pl.multiple_of(at * patches, patches), patches), :] = kept.astype(BF)
        return 0

    def prepare():
        def source(shape, dim):
            row = iota(shape, dim)
            e = lax.rem(lax.div(row, block) + parity, 2)
            cc = lax.rem(lax.div(row, sub), 2)
            within = lax.rem(row, sub)
            return lax.div(within, ih) * tile + cc * 2 * ih + e * ih + lax.rem(within, ih)

        perm[...] = (source(perm.shape, 0) == iota(perm.shape, 1)).astype(BF)
        permt[...] = (source(perm.shape, 1) == iota(perm.shape, 0)).astype(BF)
        for half in range(HALVES):
            for j in range(2 * nch):
                pre[half, j] = jnp.zeros((4 * sub, DC), F32)

    def prepare_later():
        lax.fori_loop(0, images, mix_weights, 0)
        downb_in.wait()
        shape = (2 * block, n_exp)
        n_row = 2 * k_own + lax.rem(lax.div(iota(shape, 0), block) + parity, 2)
        pick = (n_row == iota(shape, 1)).astype(BF)
        first = lax.rem(lax.div(iota((2 * block, LN), 0), sub), 2) == 0
        for c in range(nch):
            both = dot(pick, downb_ref[:, c * DC : (c + 1) * DC])
            bias_rows[c] = jnp.where(first, both[:, :LN], both[:, LN:]).astype(BF)

    def run(first, last, *steps):
        def one(t, _):
            for step, shift in steps:
                step(t + shift)
            return 0

        lax.fori_loop(first, last, one, 0)

    ahead = units - 3
    sends_w[2].start()
    run(0, nch, (dispatch, 0))
    soften(range(ih, images))
    run(nch, ahead, (dispatch, 0))
    sends_w[0].start()
    sends_w[1].start()
    prepare()
    prepare_later()
    run(0, 3, (spread_x, 0), (dispatch, ahead))
    up_in.wait()
    sends_w[0].wait_recv()
    run(0, nch, (spread_x, 3), (up, 0))
    upb_in.wait()
    sends_w[2].wait_recv()
    spread_x(nch + 3)
    activate(0)
    spread_x(nch + 4)
    down_in.wait()
    sends_w[1].wait_recv()
    run(0, nch, (down, 0))

    run(0, nch, (up, nch))
    activate(1)
    run(0, nch, (down, nch), (finish, 0))
    run(0, nch, (finish, nch), (mix, 0))
    run(nch, units, (mix, 0))

    def drain(buf, first, count, sem):
        view = buf.at[:, pl.ds(first, count)]
        pltpu.make_async_copy(view, view, sem).wait()

    for copy in sends_w:
        copy.wait_send()
    drain(slots_s, 0, nk - 1, s1_sem)
    drain(rows, 1, 3, s2_sem)
    drain(part_s, 1, 3, s3_sem)
    drain(fin, 0, nk - 1, s4_sem)


def body(tokens, slot_keys, logit_scale, up_weight, up_bias, down_weight, down_bias):
    images, patches, width = tokens.shape
    nk = lax.axis_size("expert") // 2
    nch = width // DC
    n_exp = 2 * nk
    ih = images // HALVES
    tile = 4 * ih
    cols = nk * tile
    sub = nk * ih
    units = HALVES * nch
    hid = up_weight.shape[2]
    dma = pltpu.SemaphoreType.DMA
    vmem = pl.BlockSpec(memory_space=pltpu.VMEM)
    hbm = pl.BlockSpec(memory_space=pltpu.HBM)
    return pl.pallas_call(
        functools.partial(exchange_kernel, nk, nch),
        out_shape=pltpu.VMEM(tokens.shape, BF),
        in_specs=[hbm] * 7,
        out_specs=vmem,
        scratch_shapes=[
            pltpu.VMEM((images, patches, width), BF),
            pltpu.VMEM((n_exp, width), BF),
            pltpu.SMEM((1,), F32),
            pltpu.VMEM((1, hid), BF),
            pltpu.VMEM((n_exp, width), BF),
            pltpu.VMEM((HALVES, 2, cols, ih * patches), BF),
            pltpu.VMEM((width, cols), BF),
            pltpu.VMEM((images * patches, cols), F32),
            pltpu.VMEM((4 * sub, 4 * sub), BF),
            pltpu.VMEM((4 * sub, 4 * sub), BF),
            pltpu.VMEM((2, width, hid), BF),
            pltpu.VMEM((2, hid, width), BF),
            pltpu.VMEM((1, hid), BF),
            pltpu.VMEM((nch, 4 * sub, LN), BF),
            pltpu.VMEM((units, nk, tile, LN), BF),
            pltpu.VMEM((units, nk, tile, LN), BF),
            pltpu.VMEM((units, 5, 2 * sub, LN), BF),
            pltpu.VMEM((HALVES, 2 * nch, 4 * sub, DC), F32),
            pltpu.VMEM((HALVES, 4 * sub, 2 * hid), BF),
            pltpu.VMEM((units, 4, 2 * sub, LN), BF),
            pltpu.VMEM((units, 4, 2 * sub, LN), BF),
            pltpu.VMEM((units, nk, tile, LN), BF),
            pltpu.VMEM((HALVES, 2, ih * patches, cols), BF),
            pltpu.VMEM((units, nk, tile, LN), BF),
            dma((images,)),
            dma((6,)),
            dma((3,)),
            dma((3,)),
            dma,
            dma((units,)),
            dma,
            dma((units,)),
            dma,
            dma((units,)),
            dma,
            dma((units,)),
        ],
        compiler_params=pltpu.CompilerParams(
            collective_id=0, has_side_effects=True, vmem_limit_bytes=58 * 1024 * 1024
        ),
        name="exchange",
    )(tokens, slot_keys.T, logit_scale, up_weight, up_bias, down_weight, down_bias)


def solution(mesh):
    return jax.shard_map(
        body,
        mesh=mesh,
        in_specs=(
            P(("dp", "expert"), None, None),
            P(),
            P(),
            P("expert", None, "dp"),
            P("expert", "dp"),
            P("expert", "dp", None),
            P(),
        ),
        out_specs=P(("dp", "expert"), None, None),
        check_vma=False,
    )
```

```python
import functools

import jax
import jax.numpy as jnp
from jax import lax
from jax.experimental import pallas as pl
from jax.experimental.pallas import tpu as pltpu
from jax.sharding import PartitionSpec as P

norm_eps = 1e-06
MESH = pl.DeviceIdType.MESH
LN = 128
DC = 2 * LN
HALVES = 2
BF = jnp.bfloat16
F32 = jnp.float32


def iota(shape, dim):
    return lax.broadcasted_iota(jnp.int32, shape, dim)


def dot(a, b):
    return jnp.dot(a, b, preferred_element_type=F32)


def offsets(nk):
    ny, nz = (4, 8) if nk == 32 else (1, nk)
    hops = lambda d, n: min(d, n - d)
    near = [(1, 2), (3, 6), (2, 1), (2, 7)] if nk == 32 else []
    key = lambda o: (hops(o[0], ny) + hops(o[1], nz), o not in near, hops(o[1], nz))
    return ny, nz, sorted([(dy, dz) for dy in range(ny) for dz in range(nz)], key=key)


def exchange_kernel(
    nk,
    nch,
    tok_hbm,
    keys_hbm,
    scale_hbm,
    up_hbm,
    upb_hbm,
    down_hbm,
    downb_hbm,
    out_ref,
    tok,
    keys_ref,
    scale_ref,
    upb_ref,
    downb_ref,
    disp_t,
    keyrep,
    scores,
    perm,
    permt,
    wup,
    wdown,
    bup,
    bias_rows,
    slots_s,
    slots_r,
    rows,
    pre,
    hidden,
    joined,
    part_s,
    part_r,
    fin,
    comb,
    got,
    tok_sem,
    load_sem,
    wsend_sem,
    wrecv_sem,
    s1_sem,
    r1_sem,
    s2_sem,
    r2_sem,
    s3_sem,
    r3_sem,
    s4_sem,
    r4_sem,
):
    images, patches, width = tok.shape
    ih = images // HALVES
    tile = 4 * ih
    sub = nk // 2 * ih
    block = 2 * sub
    n_exp = keys_ref.shape[0]
    units = HALVES * nch
    own = lax.axis_index("expert")
    dp = lax.axis_index("dp")
    k_own = lax.div(own, 2)
    parity = lax.rem(own, 2)
    flip = own + 1 - 2 * parity
    far = lax.rem(dp + 2, 4)
    core = dp + 1 - 2 * lax.rem(dp, 2)
    members = ((dp, own), (dp, flip), (far, flip), (far, own))

    ny, nz, order = offsets(nk)
    y_own, z_own = lax.div(k_own, nz), lax.rem(k_own, nz)
    near = nk // 2

    def peer(pos, sign=1):
        dy, dz = order[pos]
        y = lax.rem(y_own + (sign * dy) % ny, ny)
        z = lax.rem(z_own + (sign * dz) % nz, nz)
        k = y * nz + z
        return k, {"dp": dp, "expert": 2 * k + parity}

    tok_in = [
        pltpu.make_async_copy(tok_hbm.at[i], tok.at[i], tok_sem.at[i]) for i in range(images)
    ]
    keys_in = pltpu.make_async_copy(keys_hbm, keys_ref, load_sem.at[2])
    scale_in = pltpu.make_async_copy(scale_hbm, scale_ref, load_sem.at[3])
    upb_in = pltpu.make_async_copy(upb_hbm, upb_ref, load_sem.at[4])
    downb_in = pltpu.make_async_copy(downb_hbm, downb_ref, load_sem.at[5])
    for copy in (keys_in, scale_in, *tok_in, upb_in, downb_in):
        copy.start()
    up_in = pltpu.make_async_copy(up_hbm.at[0], wup.at[0], load_sem.at[0])
    down_in = pltpu.make_async_copy(down_hbm.at[0], wdown.at[0], load_sem.at[1])
    up_in.start()
    down_in.start()

    barrier = pltpu.get_barrier_semaphore()

    def greet(pos, _):
        _, where = peer(pos)
        pl.semaphore_signal(barrier, inc=1, device_id=where, device_id_type=MESH)
        return 0

    for pos in reversed(range(1, nk)):
        greet(pos, 0)
    for d, e in members[1:]:
        pl.semaphore_signal(barrier, inc=1, device_id={"dp": d, "expert": e}, device_id_type=MESH)
    pl.semaphore_signal(barrier, inc=1, device_id={"dp": core, "expert": own}, device_id_type=MESH)

    keys_in.wait()
    keys = keys_ref[...].astype(F32)
    keys = keys * lax.rsqrt(jnp.mean(keys * keys, axis=1, keepdims=True) + norm_eps)
    col = iota((nk * tile, n_exp), 0)
    col = 2 * lax.div(col, tile) + lax.rem(lax.div(col, ih), 2)
    spread = (col == iota((nk * tile, n_exp), 1)).astype(BF)
    keyrep[...] = jnp.transpose(dot(spread, keys.astype(BF))).astype(BF)

    def place_mask(shape, dim, i, cc):
        at = iota(shape, dim)
        return (lax.rem(at, ih) == i) & (lax.rem(lax.div(at, 2 * ih), 2) == cc)

    scale_in.wait()
    scale = scale_ref[0]

    def soften(images_of):
        for i in images_of:
            tok_in[i].wait()
            t = tok[i]
            tf = t.astype(F32)
            factor = lax.rsqrt(jnp.mean(tf * tf, axis=1, keepdims=True) + norm_eps)
            logits = scale * (dot(t, keyrep[...]) * factor) / width
            scores[pl.ds(i * patches, patches), :] = logits
            e_tok = jnp.exp(logits - jnp.max(logits, axis=0, keepdims=True))
            share = jnp.transpose(e_tok / jnp.sum(e_tok, axis=0, keepdims=True))
            half, at = divmod(i, ih)
            for cc in range(2):
                kept = jnp.where(place_mask(share.shape, 0, at, cc), share, 0.0)
                disp_t[half, cc, :, pl.ds(at * patches, patches)] = kept.astype(BF)

    soften(range(ih))

    pl.semaphore_wait(barrier, nk - 1 + 4)

    where_core = {"dp": core, "expert": own}
    sends_w = []
    for j, (src_ref, dst_ref) in enumerate(
        ((up_hbm.at[0], wup.at[1]), (down_hbm.at[0], wdown.at[1]), (upb_hbm, bup))
    ):
        sends_w.append(
            pltpu.make_async_remote_copy(
                src_ref=src_ref,
                dst_ref=dst_ref,
                send_sem=wsend_sem.at[j],
                recv_sem=wrecv_sem.at[j],
                device_id=where_core,
                device_id_type=MESH,
            )
        )

    def lanes(c):
        return pl.ds(pl.multiple_of(c * DC, DC), DC)

    def lane_tile(c, cc):
        return pl.ds(pl.multiple_of(c * DC + cc * LN, LN), LN)

    def of(u):
        half = lax.div(u, nch)
        return half, u - half * nch

    def groups(part):
        return range(nk - 1, near - 1, -1) if part else range(near - 1, 0, -1)

    def compute_slots(u):
        half, c = of(u)
        ts = tok[pl.ds(half * ih, ih), :, lanes(c)].reshape(ih * patches, DC)
        s = dot(disp_t[half, 0], ts[:, :LN]) + dot(disp_t[half, 1], ts[:, LN:])
        slots_s[u] = s.reshape(nk, tile, LN).astype(BF)
        slots_r[u, 0] = slots_s[u, k_own]

    def send_slots(u, part):
        for pos in groups(part):
            k, where = peer(pos)
            pltpu.make_async_remote_copy(
                src_ref=slots_s.at[u, k],
                dst_ref=slots_r.at[u, pos],
                send_sem=s1_sem,
                recv_sem=r1_sem.at[u, part],
                device_id=where,
                device_id_type=MESH,
            ).start()

    def dispatch_near(u):
        compute_slots(u)
        send_slots(u, 0)

    def dispatch_far(u):
        send_slots(u, 1)

    def dispatch(u):
        compute_slots(u)
        send_slots(u, 1)
        send_slots(u, 0)

    def send_back(u, part):
        for pos in groups(part):
            k, where = peer(pos, -1)
            pltpu.make_async_remote_copy(
                src_ref=fin.at[u, pos],
                dst_ref=got.at[u, k_own],
                send_sem=s4_sem,
                recv_sem=r4_sem.at[u],
                device_id=where,
                device_id_type=MESH,
            ).start()

    def to_member(src_ref, dst_ref, m, s_sem, r_sem):
        d, e = members[m]
        return pltpu.make_async_remote_copy(
            src_ref=src_ref,
            dst_ref=dst_ref,
            send_sem=s_sem,
            recv_sem=r_sem,
            device_id={"dp": d, "expert": e},
            device_id_type=MESH,
        )

    def spread_x(u, part):
        count = near if part else near - 1
        view = slots_r.at[u, pl.ds(nk - count if part else 1, count)]
        if count:
            pltpu.make_async_copy(view, view, r1_sem.at[u, part]).wait()
        tiles = slots_r[u, pl.ds(part * near, near)].reshape(2 * block, LN)
        moved = dot(perm[...], tiles).astype(BF)
        rows[u, part, 0] = moved[:block]
        rows[u, part, 4] = moved[block:]
        for m, piece in ((3, 0), (1, 4), (2, 4)):
            to_member(
                rows.at[u, part, piece], rows.at[u, part, m], m, s2_sem, r2_sem.at[u]
            ).start()

    def up(u):
        half, c = of(u)
        view = rows.at[u, pl.ds(0, 2), pl.ds(1, 3)]
        pltpu.make_async_copy(view, view, r2_sem.at[u]).wait()
        x = jnp.concatenate(
            [rows[u, :, pl.ds(0, 4), pl.ds(0, sub)], rows[u, :, pl.ds(0, 4), pl.ds(sub, sub)]],
            axis=3,
        ).reshape(8 * sub, DC)
        for j in range(2 * nch):
            which, at = divmod(j, nch)
            pre[half, j] += dot(x, wup[which, lanes(c), at * DC : (at + 1) * DC])

    def activate(half):
        for which, bias_ref in ((0, upb_ref), (1, bup)):

            def one(j, _, which=which, bias_ref=bias_ref):
                v = pre[half, which * nch + j] + bias_ref[:, lanes(j)].astype(F32)
                h = 0.5 * v * (1.0 + lax.erf(v * (2.0**-0.5)))
                hidden[half, :, lanes(which * nch + j)] = h.astype(BF)
                return 0

            lax.fori_loop(0, nch, one, 0)

    def join(half):
        for c in range(nch):
            view = rows.at[half * nch + c, pl.ds(0, 2), pl.ds(1, 3)]
            pltpu.make_async_copy(view, view, r2_sem.at[half * nch + c]).wait()
        pieces = [
            rows[half * nch + c, :, pl.ds(0, 4), pl.ds(cc * sub, sub)]
            for c in range(nch)
            for cc in range(2)
        ]
        joined[...] = jnp.concatenate(pieces, axis=3).reshape(8 * sub, width)

    def up_and_activate(half, which, bias_ref):
        for j in range(nch):
            cols = slice(j * DC, (j + 1) * DC)
            v = dot(joined[...], wup[which, :, cols]) + bias_ref[:, cols].astype(F32)
            h = 0.5 * v * (1.0 + lax.erf(v * (2.0**-0.5)))
            hidden[half, :, which * width + j * DC : which * width + (j + 1) * DC] = h.astype(BF)

    def down(u):
        half, c = of(u)
        p = dot(hidden[half], wdown[:, :, lanes(c)].reshape(2 * width, DC)).astype(BF)
        part_s[u, :, :, pl.ds(0, sub)] = p[:, :LN].reshape(2, 4, sub, LN)
        part_s[u, :, :, pl.ds(sub, sub)] = p[:, LN:].reshape(2, 4, sub, LN)

    def send_part(u, part):
        for m in (3, 1, 2):
            to_member(
                part_s.at[u, part, m], part_r.at[u, part, m], m, s3_sem, r3_sem.at[u, part]
            ).start()

    def down_both(u):
        down(u)
        send_part(u, 1)
        send_part(u, 0)

    def down_far(u):
        down(u)
        send_part(u, 1)

    def finish(u, part):
        half, c = of(u)
        view = part_r.at[u, part, pl.ds(1, 3)]
        pltpu.make_async_copy(view, view, r3_sem.at[u, part]).wait()
        mine = part_s[u, part, 0].astype(F32) + part_r[u, part, 3].astype(F32)
        other = part_r[u, part, 1].astype(F32) + part_r[u, part, 2].astype(F32)
        total = jnp.concatenate([mine, other], axis=0) + bias_rows[c].astype(F32)
        moved = dot(permt[...], total.astype(BF)).reshape(near, tile, LN).astype(BF)
        fin[u, pl.ds(part * near, near)] = moved
        if part == 0:
            got[u, k_own] = fin[u, 0]
        send_back(u, part)

    def mix(u):
        half, c = of(u)
        view = got.at[u, pl.ds(0, nk - 1)]
        pltpu.make_async_copy(view, view, r4_sem.at[u]).wait()
        back = got[u].reshape(nk * tile, LN)
        for at in range(ih):
            for cc in range(2):
                mixed = dot(comb[half, cc, pl.ds(at * patches, patches), :], back)
                out_ref[half * ih + at, :, lane_tile(c, cc)] = mixed.astype(BF)

    def mix_weights(i, _):
        logits = scores[pl.ds(pl.multiple_of(i * patches, patches), patches), :]
        half = lax.div(i, ih)
        at = lax.rem(i, ih)
        masks = [place_mask(logits.shape, 1, at, cc) for cc in range(2)]
        e_slot = jnp.exp(logits - jnp.max(logits, axis=1, keepdims=True))
        total = jnp.sum(jnp.where(masks[0], e_slot, 0.0), axis=1, keepdims=True)
        share = e_slot / total
        for cc in range(2):
            kept = jnp.where(masks[cc], share, 0.0)
            comb[half, cc, pl.ds(pl.multiple_of(at * patches, patches), patches), :] = kept.astype(BF)
        return 0

    def prepare():
        def source(shape, dim):
            row = iota(shape, dim)
            e = lax.rem(lax.div(row, block) + parity, 2)
            cc = lax.rem(lax.div(row, sub), 2)
            within = lax.rem(row, sub)
            return lax.div(within, ih) * tile + cc * 2 * ih + e * ih + lax.rem(within, ih)

        perm[...] = (source(perm.shape, 0) == iota(perm.shape, 1)).astype(BF)
        permt[...] = (source(perm.shape, 1) == iota(perm.shape, 0)).astype(BF)
        for half in range(HALVES):
            for j in range(2 * nch):
                pre[half, j] = jnp.zeros((8 * sub, DC), F32)

    def prepare_later():
        lax.fori_loop(0, images, mix_weights, 0)
        downb_in.wait()
        shape = (2 * block, n_exp)
        n_row = 2 * k_own + lax.rem(lax.div(iota(shape, 0), block) + parity, 2)
        pick = (n_row == iota(shape, 1)).astype(BF)
        first = lax.rem(lax.div(iota((2 * block, LN), 0), sub), 2) == 0
        for c in range(nch):
            both = dot(pick, downb_ref[:, c * DC : (c + 1) * DC])
            bias_rows[c] = jnp.where(first, both[:, :LN], both[:, LN:]).astype(BF)

    def run(first, last, *steps):
        def one(t, _):
            for step, shift in steps:
                step(t + shift)
            return 0

        lax.fori_loop(first, last, one, 0)

    sends_w[2].start()
    run(0, nch, (dispatch_near, 0))
    run(0, nch, (dispatch_far, 0))
    sends_w[0].start()
    sends_w[1].start()
    prepare()
    soften(range(ih, images))

    def spread_near(u):
        spread_x(u, 0)

    def spread_far(u):
        spread_x(u, 1)

    def spread_both(u):
        spread_x(u, 1)
        spread_x(u, 0)

    run(0, nch, (dispatch, nch), (spread_near, 0))
    prepare_later()
    up_in.wait()
    sends_w[0].wait_recv()
    run(0, 3, (spread_far, 0))
    run(0, 2, (spread_far, 3), (up, 0))
    run(0, 3, (spread_both, nch), (up, 2))
    upb_in.wait()
    sends_w[2].wait_recv()
    spread_both(nch + 3)
    activate(0)
    spread_both(nch + 4)
    down_in.wait()
    sends_w[1].wait_recv()
    run(0, nch, (down_both, 0))
    def finish_near(u):
        finish(u, 0)

    def finish_far(u):
        finish(u, 1)

    def finish_both(u):
        finish(u, 1)
        finish(u, 0)

    def finish_next(t):
        @pl.when(t + 1 < nch)
        def _():
            finish_both(t + 1)

    join(1)
    up_and_activate(1, 0, upb_ref)
    run(0, 1, (finish_both, 0))
    up_and_activate(1, 1, bup)
    run(0, nch, (finish_next, 0), (down_far, nch))
    for c in range(nch):
        send_part(nch + c, 0)
    run(0, nch, (finish_far, nch))
    run(0, nch, (finish_near, nch))
    run(0, units, (mix, 0))

    def drain(buf, first, count, sem):
        view = buf.at[:, pl.ds(first, count)]
        pltpu.make_async_copy(view, view, sem).wait()

    for copy in sends_w:
        copy.wait_send()
    drain(slots_s, 0, nk - 1, s1_sem)
    for buf, sem in ((rows, s2_sem), (part_s, s3_sem)):
        view = buf.at[:, :, pl.ds(1, 3)]
        pltpu.make_async_copy(view, view, sem).wait()
    drain(fin, 0, nk - 1, s4_sem)


def body(tokens, slot_keys, logit_scale, up_weight, up_bias, down_weight, down_bias):
    images, patches, width = tokens.shape
    nk = lax.axis_size("expert") // 2
    nch = width // DC
    n_exp = 2 * nk
    ih = images // HALVES
    tile = 4 * ih
    cols = nk * tile
    sub = nk // 2 * ih
    units = HALVES * nch
    hid = up_weight.shape[2]
    dma = pltpu.SemaphoreType.DMA
    vmem = pl.BlockSpec(memory_space=pltpu.VMEM)
    hbm = pl.BlockSpec(memory_space=pltpu.HBM)
    return pl.pallas_call(
        functools.partial(exchange_kernel, nk, nch),
        out_shape=pltpu.VMEM(tokens.shape, BF),
        in_specs=[hbm] * 7,
        out_specs=vmem,
        scratch_shapes=[
            pltpu.VMEM((images, patches, width), BF),
            pltpu.VMEM((n_exp, width), BF),
            pltpu.SMEM((1,), F32),
            pltpu.VMEM((1, hid), BF),
            pltpu.VMEM((n_exp, width), BF),
            pltpu.VMEM((HALVES, 2, cols, ih * patches), BF),
            pltpu.VMEM((width, cols), BF),
            pltpu.VMEM((images * patches, cols), F32),
            pltpu.VMEM((4 * sub, 4 * sub), BF),
            pltpu.VMEM((4 * sub, 4 * sub), BF),
            pltpu.VMEM((2, width, hid), BF),
            pltpu.VMEM((2, hid, width), BF),
            pltpu.VMEM((1, hid), BF),
            pltpu.VMEM((nch, 4 * sub, LN), BF),
            pltpu.VMEM((units, nk, tile, LN), BF),
            pltpu.VMEM((units, nk, tile, LN), BF),
            pltpu.VMEM((units, 2, 5, 2 * sub, LN), BF),
            pltpu.VMEM((HALVES, 2 * nch, 8 * sub, DC), F32),
            pltpu.VMEM((HALVES, 8 * sub, 2 * hid), BF),
            pltpu.VMEM((8 * sub, width), BF),
            pltpu.VMEM((units, 2, 4, 2 * sub, LN), BF),
            pltpu.VMEM((units, 2, 4, 2 * sub, LN), BF),
            pltpu.VMEM((units, nk, tile, LN), BF),
            pltpu.VMEM((HALVES, 2, ih * patches, cols), BF),
            pltpu.VMEM((units, nk, tile, LN), BF),
            dma((images,)),
            dma((6,)),
            dma((3,)),
            dma((3,)),
            dma,
            dma((units, 2)),
            dma,
            dma((units,)),
            dma,
            dma((units, 2)),
            dma,
            dma((units,)),
        ],
        compiler_params=pltpu.CompilerParams(
            collective_id=0, has_side_effects=True, vmem_limit_bytes=58 * 1024 * 1024
        ),
        name="exchange",
    )(tokens, slot_keys.T, logit_scale, up_weight, up_bias, down_weight, down_bias)


def solution(mesh):
    return jax.shard_map(
        body,
        mesh=mesh,
        in_specs=(
            P(("dp", "expert"), None, None),
            P(),
            P(),
            P("expert", None, "dp"),
            P("expert", "dp"),
            P("expert", "dp", None),
            P(),
        ),
        out_specs=P(("dp", "expert"), None, None),
        check_vma=False,
    )
```

```python
import functools

import jax
import jax.numpy as jnp
from jax import lax
from jax.experimental import pallas as pl
from jax.experimental.pallas import tpu as pltpu
from jax.sharding import PartitionSpec as P

norm_eps = 1e-06
MESH = pl.DeviceIdType.MESH
LN = 128
DC = 2 * LN
HALVES = 2
BF = jnp.bfloat16
F32 = jnp.float32


def iota(shape, dim):
    return lax.broadcasted_iota(jnp.int32, shape, dim)


def dot(a, b):
    return jnp.dot(a, b, preferred_element_type=F32)


def offsets(nk):
    ny, nz = (4, 8) if nk == 32 else (1, nk)
    hops = lambda d, n: min(d, n - d)
    near = [(1, 2), (3, 6), (2, 1), (2, 7)] if nk == 32 else []
    key = lambda o: (hops(o[0], ny) + hops(o[1], nz), o not in near, hops(o[1], nz))
    return ny, nz, sorted([(dy, dz) for dy in range(ny) for dz in range(nz)], key=key)


def exchange_kernel(
    nk,
    nch,
    tok_hbm,
    keys_hbm,
    scale_hbm,
    up_hbm,
    upb_hbm,
    down_hbm,
    downb_hbm,
    out_ref,
    tok,
    keys_ref,
    scale_ref,
    upb_ref,
    downb_ref,
    disp_t,
    keyrep,
    scores,
    perm,
    permt,
    wup,
    wdown,
    bup,
    bias_rows,
    slots_s,
    slots_r,
    rows,
    pre,
    hidden,
    joined,
    part_s,
    part_r,
    fin,
    comb,
    got,
    tok_sem,
    load_sem,
    wsend_sem,
    wrecv_sem,
    s1_sem,
    r1_sem,
    s2_sem,
    r2_sem,
    s3_sem,
    r3_sem,
    s4_sem,
    r4_sem,
):
    images, patches, width = tok.shape
    ih = images // HALVES
    tile = 4 * ih
    sub = nk // 2 * ih
    block = 2 * sub
    n_exp = keys_ref.shape[0]
    units = HALVES * nch
    own = lax.axis_index("expert")
    dp = lax.axis_index("dp")
    k_own = lax.div(own, 2)
    parity = lax.rem(own, 2)
    flip = own + 1 - 2 * parity
    far = lax.rem(dp + 2, 4)
    core = dp + 1 - 2 * lax.rem(dp, 2)
    members = ((dp, own), (dp, flip), (far, flip), (far, own))

    ny, nz, order = offsets(nk)
    y_own, z_own = lax.div(k_own, nz), lax.rem(k_own, nz)
    near = nk // 2

    def peer(pos, sign=1):
        dy, dz = order[pos]
        y = lax.rem(y_own + (sign * dy) % ny, ny)
        z = lax.rem(z_own + (sign * dz) % nz, nz)
        k = y * nz + z
        return k, {"dp": dp, "expert": 2 * k + parity}

    tok_in = [
        pltpu.make_async_copy(tok_hbm.at[i], tok.at[i], tok_sem.at[i]) for i in range(images)
    ]
    keys_in = pltpu.make_async_copy(keys_hbm, keys_ref, load_sem.at[2])
    scale_in = pltpu.make_async_copy(scale_hbm, scale_ref, load_sem.at[3])
    upb_in = pltpu.make_async_copy(upb_hbm, upb_ref, load_sem.at[4])
    downb_in = pltpu.make_async_copy(downb_hbm, downb_ref, load_sem.at[5])
    for copy in (keys_in, scale_in, *tok_in, upb_in, downb_in):
        copy.start()
    up_in = pltpu.make_async_copy(up_hbm.at[0], wup.at[0], load_sem.at[0])
    down_in = pltpu.make_async_copy(down_hbm.at[0], wdown.at[0], load_sem.at[1])
    up_in.start()
    down_in.start()

    barrier = pltpu.get_barrier_semaphore()

    def greet(pos, _):
        _, where = peer(pos)
        pl.semaphore_signal(barrier, inc=1, device_id=where, device_id_type=MESH)
        return 0

    for pos in reversed(range(1, nk)):
        greet(pos, 0)
    for d, e in members[1:]:
        pl.semaphore_signal(barrier, inc=1, device_id={"dp": d, "expert": e}, device_id_type=MESH)
    pl.semaphore_signal(barrier, inc=1, device_id={"dp": core, "expert": own}, device_id_type=MESH)

    keys_in.wait()
    keys = keys_ref[...].astype(F32)
    keys = keys * lax.rsqrt(jnp.mean(keys * keys, axis=1, keepdims=True) + norm_eps)
    col = iota((nk * tile, n_exp), 0)
    col = 2 * lax.div(col, tile) + lax.rem(lax.div(col, ih), 2)
    spread = (col == iota((nk * tile, n_exp), 1)).astype(BF)
    keyrep[...] = jnp.transpose(dot(spread, keys.astype(BF))).astype(BF)

    def place_mask(shape, dim, i, cc):
        at = iota(shape, dim)
        return (lax.rem(at, ih) == i) & (lax.rem(lax.div(at, 2 * ih), 2) == cc)

    scale_in.wait()
    scale = scale_ref[0]

    def soften(images_of):
        for i in images_of:
            tok_in[i].wait()
            t = tok[i]
            tf = t.astype(F32)
            factor = lax.rsqrt(jnp.mean(tf * tf, axis=1, keepdims=True) + norm_eps)
            logits = scale * (dot(t, keyrep[...]) * factor) / width
            scores[pl.ds(i * patches, patches), :] = logits
            e_tok = jnp.exp(logits - jnp.max(logits, axis=0, keepdims=True))
            share = jnp.transpose(e_tok / jnp.sum(e_tok, axis=0, keepdims=True))
            half, at = divmod(i, ih)
            for cc in range(2):
                kept = jnp.where(place_mask(share.shape, 0, at, cc), share, 0.0)
                disp_t[half, cc, :, pl.ds(at * patches, patches)] = kept.astype(BF)

    soften(range(ih))

    pl.semaphore_wait(barrier, nk - 1 + 4)

    where_core = {"dp": core, "expert": own}
    sends_w = []
    for j, (src_ref, dst_ref) in enumerate(
        ((up_hbm.at[0], wup.at[1]), (down_hbm.at[0], wdown.at[1]), (upb_hbm, bup))
    ):
        sends_w.append(
            pltpu.make_async_remote_copy(
                src_ref=src_ref,
                dst_ref=dst_ref,
                send_sem=wsend_sem.at[j],
                recv_sem=wrecv_sem.at[j],
                device_id=where_core,
                device_id_type=MESH,
            )
        )

    def lanes(c):
        return pl.ds(pl.multiple_of(c * DC, DC), DC)

    def lane_tile(c, cc):
        return pl.ds(pl.multiple_of(c * DC + cc * LN, LN), LN)

    def of(u):
        half = lax.div(u, nch)
        return half, u - half * nch

    def groups(part):
        return range(nk - 1, near - 1, -1) if part else range(near - 1, 0, -1)

    def compute_slots(u):
        half, c = of(u)
        ts = tok[pl.ds(half * ih, ih), :, lanes(c)].reshape(ih * patches, DC)
        s = dot(disp_t[half, 0], ts[:, :LN]) + dot(disp_t[half, 1], ts[:, LN:])
        slots_s[u] = s.reshape(nk, tile, LN).astype(BF)
        slots_r[u, 0] = slots_s[u, k_own]

    def send_slots(u, part):
        for pos in groups(part):
            k, where = peer(pos)
            pltpu.make_async_remote_copy(
                src_ref=slots_s.at[u, k],
                dst_ref=slots_r.at[u, pos],
                send_sem=s1_sem,
                recv_sem=r1_sem.at[u, part],
                device_id=where,
                device_id_type=MESH,
            ).start()

    def dispatch_near(u):
        compute_slots(u)
        send_slots(u, 0)

    def dispatch_far(u):
        send_slots(u, 1)

    def dispatch(u):
        compute_slots(u)
        send_slots(u, 1)
        send_slots(u, 0)

    def send_back(u, part):
        for pos in groups(part):
            k, where = peer(pos, -1)
            pltpu.make_async_remote_copy(
                src_ref=fin.at[u, pos],
                dst_ref=got.at[u, k_own],
                send_sem=s4_sem,
                recv_sem=r4_sem.at[u],
                device_id=where,
                device_id_type=MESH,
            ).start()

    def to_member(src_ref, dst_ref, m, s_sem, r_sem):
        d, e = members[m]
        return pltpu.make_async_remote_copy(
            src_ref=src_ref,
            dst_ref=dst_ref,
            send_sem=s_sem,
            recv_sem=r_sem,
            device_id={"dp": d, "expert": e},
            device_id_type=MESH,
        )

    def spread_x(u, part):
        count = near if part else near - 1
        view = slots_r.at[u, pl.ds(nk - count if part else 1, count)]
        if count:
            pltpu.make_async_copy(view, view, r1_sem.at[u, part]).wait()
        tiles = slots_r[u, pl.ds(part * near, near)].reshape(2 * block, LN)
        moved = dot(perm[...], tiles).astype(BF)
        rows[u, part, 0] = moved[:block]
        rows[u, part, 4] = moved[block:]
        for m, piece in ((3, 0), (1, 4), (2, 4)):
            to_member(
                rows.at[u, part, piece], rows.at[u, part, m], m, s2_sem, r2_sem.at[u]
            ).start()

    def up(u):
        half, c = of(u)
        view = rows.at[u, pl.ds(0, 2), pl.ds(1, 3)]
        pltpu.make_async_copy(view, view, r2_sem.at[u]).wait()
        x = jnp.concatenate(
            [rows[u, :, pl.ds(0, 4), pl.ds(0, sub)], rows[u, :, pl.ds(0, 4), pl.ds(sub, sub)]],
            axis=3,
        ).reshape(8 * sub, DC)
        for j in range(2 * nch):
            which, at = divmod(j, nch)
            pre[half, j] += dot(x, wup[which, lanes(c), at * DC : (at + 1) * DC])

    def activate(half):
        for which, bias_ref in ((0, upb_ref), (1, bup)):

            def one(j, _, which=which, bias_ref=bias_ref):
                v = pre[half, which * nch + j] + bias_ref[:, lanes(j)].astype(F32)
                h = 0.5 * v * (1.0 + lax.erf(v * (2.0**-0.5)))
                hidden[half, :, lanes(which * nch + j)] = h.astype(BF)
                return 0

            lax.fori_loop(0, nch, one, 0)

    def join(half):
        for c in range(nch):
            view = rows.at[half * nch + c, pl.ds(0, 2), pl.ds(1, 3)]
            pltpu.make_async_copy(view, view, r2_sem.at[half * nch + c]).wait()
        pieces = [
            rows[half * nch + c, :, pl.ds(0, 4), pl.ds(cc * sub, sub)]
            for c in range(nch)
            for cc in range(2)
        ]
        joined[...] = jnp.concatenate(pieces, axis=3).reshape(8 * sub, width)

    def up_and_activate(half, which, bias_ref):
        for j in range(nch):
            cols = slice(j * DC, (j + 1) * DC)
            v = dot(joined[...], wup[which, :, cols]) + bias_ref[:, cols].astype(F32)
            h = 0.5 * v * (1.0 + lax.erf(v * (2.0**-0.5)))
            hidden[half, :, which * width + j * DC : which * width + (j + 1) * DC] = h.astype(BF)

    def down(u):
        half, c = of(u)
        p = dot(hidden[half], wdown[:, :, lanes(c)].reshape(2 * width, DC)).astype(BF)
        part_s[u, :, :, pl.ds(0, sub)] = p[:, :LN].reshape(2, 4, sub, LN)
        part_s[u, :, :, pl.ds(sub, sub)] = p[:, LN:].reshape(2, 4, sub, LN)

    def send_part(u, part):
        for m in (3, 1, 2):
            to_member(
                part_s.at[u, part, m], part_r.at[u, part, m], m, s3_sem, r3_sem.at[u, part]
            ).start()

    def down_both(u):
        down(u)
        send_part(u, 1)
        send_part(u, 0)

    def down_far(u):
        down(u)
        send_part(u, 1)

    def finish(u, part):
        half, c = of(u)
        view = part_r.at[u, part, pl.ds(1, 3)]
        pltpu.make_async_copy(view, view, r3_sem.at[u, part]).wait()
        mine = part_s[u, part, 0].astype(F32) + part_r[u, part, 3].astype(F32)
        other = part_r[u, part, 1].astype(F32) + part_r[u, part, 2].astype(F32)
        total = jnp.concatenate([mine, other], axis=0) + bias_rows[c].astype(F32)
        moved = dot(permt[...], total.astype(BF)).reshape(near, tile, LN).astype(BF)
        fin[u, pl.ds(part * near, near)] = moved
        if part == 0:
            got[u, k_own] = fin[u, 0]
        send_back(u, part)

    def mix(u):
        half, c = of(u)
        view = got.at[u, pl.ds(0, nk - 1)]
        pltpu.make_async_copy(view, view, r4_sem.at[u]).wait()
        back = got[u].reshape(nk * tile, LN)
        for at in range(ih):
            for cc in range(2):
                mixed = dot(comb[half, cc, pl.ds(at * patches, patches), :], back)
                out_ref[half * ih + at, :, lane_tile(c, cc)] = mixed.astype(BF)

    def mix_pair(t):
        half = HALVES - 1
        c = 2 * t
        u = half * nch + c
        for v in range(2):
            view = got.at[u + v, pl.ds(0, nk - 1)]
            pltpu.make_async_copy(view, view, r4_sem.at[u + v]).wait()
        back = jnp.concatenate([got[u + v].reshape(nk * tile, LN) for v in range(2)], axis=1)
        for at in range(ih):
            for cc in range(2):
                mixed = dot(comb[half, cc, pl.ds(at * patches, patches), :], back).astype(BF)
                out_ref[half * ih + at, :, lane_tile(c, cc)] = mixed[:, :LN]
                out_ref[half * ih + at, :, lane_tile(c + 1, cc)] = mixed[:, LN:]

    def mix_weights(i, _):
        logits = scores[pl.ds(pl.multiple_of(i * patches, patches), patches), :]
        half = lax.div(i, ih)
        at = lax.rem(i, ih)
        masks = [place_mask(logits.shape, 1, at, cc) for cc in range(2)]
        e_slot = jnp.exp(logits - jnp.max(logits, axis=1, keepdims=True))
        total = jnp.sum(jnp.where(masks[0], e_slot, 0.0), axis=1, keepdims=True)
        share = e_slot / total
        for cc in range(2):
            kept = jnp.where(masks[cc], share, 0.0)
            comb[half, cc, pl.ds(pl.multiple_of(at * patches, patches), patches), :] = kept.astype(BF)
        return 0

    def prepare():
        def source(shape, dim):
            row = iota(shape, dim)
            e = lax.rem(lax.div(row, block) + parity, 2)
            cc = lax.rem(lax.div(row, sub), 2)
            within = lax.rem(row, sub)
            return lax.div(within, ih) * tile + cc * 2 * ih + e * ih + lax.rem(within, ih)

        perm[...] = (source(perm.shape, 0) == iota(perm.shape, 1)).astype(BF)
        permt[...] = (source(perm.shape, 1) == iota(perm.shape, 0)).astype(BF)
        for half in range(HALVES):
            for j in range(2 * nch):
                pre[half, j] = jnp.zeros((8 * sub, DC), F32)

    def prepare_later():
        lax.fori_loop(0, images, mix_weights, 0)
        downb_in.wait()
        shape = (2 * block, n_exp)
        n_row = 2 * k_own + lax.rem(lax.div(iota(shape, 0), block) + parity, 2)
        pick = (n_row == iota(shape, 1)).astype(BF)
        first = lax.rem(lax.div(iota((2 * block, LN), 0), sub), 2) == 0
        for c in range(nch):
            both = dot(pick, downb_ref[:, c * DC : (c + 1) * DC])
            bias_rows[c] = jnp.where(first, both[:, :LN], both[:, LN:]).astype(BF)

    def run(first, last, *steps):
        def one(t, _):
            for step, shift in steps:
                step(t + shift)
            return 0

        lax.fori_loop(first, last, one, 0)

    sends_w[2].start()
    run(0, nch, (dispatch_near, 0))
    run(0, nch, (dispatch_far, 0))
    sends_w[0].start()
    sends_w[1].start()
    prepare()
    soften(range(ih, images))

    def spread_near(u):
        spread_x(u, 0)

    def spread_far(u):
        spread_x(u, 1)

    def spread_both(u):
        spread_x(u, 1)
        spread_x(u, 0)

    run(0, nch, (dispatch, nch), (spread_near, 0))
    prepare_later()
    up_in.wait()
    sends_w[0].wait_recv()
    run(0, 3, (spread_far, 0))
    run(0, 2, (spread_far, 3), (up, 0))
    run(0, 3, (spread_both, nch), (up, 2))
    upb_in.wait()
    sends_w[2].wait_recv()
    spread_both(nch + 3)
    activate(0)
    spread_both(nch + 4)
    down_in.wait()
    sends_w[1].wait_recv()
    run(0, nch, (down_both, 0))
    def finish_near(u):
        finish(u, 0)

    def finish_far(u):
        finish(u, 1)

    def finish_both(u):
        finish(u, 1)
        finish(u, 0)

    def finish_next(t):
        @pl.when(t + 1 < nch)
        def _():
            finish_both(t + 1)

    join(1)
    up_and_activate(1, 0, upb_ref)
    run(0, 1, (finish_both, 0))
    up_and_activate(1, 1, bup)
    run(0, nch, (finish_next, 0), (down_far, nch))
    for c in range(nch):
        send_part(nch + c, 0)
    run(0, nch, (finish_far, nch))
    run(0, nch, (finish_near, nch))
    run(0, nch, (mix, 0))
    run(0, nch // 2, (mix_pair, 0))
    run(units - nch % 2, units, (mix, 0))

    def drain(buf, first, count, sem):
        view = buf.at[:, pl.ds(first, count)]
        pltpu.make_async_copy(view, view, sem).wait()

    for copy in sends_w:
        copy.wait_send()
    drain(slots_s, 0, nk - 1, s1_sem)
    for buf, sem in ((rows, s2_sem), (part_s, s3_sem)):
        view = buf.at[:, :, pl.ds(1, 3)]
        pltpu.make_async_copy(view, view, sem).wait()
    drain(fin, 0, nk - 1, s4_sem)


def body(tokens, slot_keys, logit_scale, up_weight, up_bias, down_weight, down_bias):
    images, patches, width = tokens.shape
    nk = lax.axis_size("expert") // 2
    nch = width // DC
    n_exp = 2 * nk
    ih = images // HALVES
    tile = 4 * ih
    cols = nk * tile
    sub = nk // 2 * ih
    units = HALVES * nch
    hid = up_weight.shape[2]
    dma = pltpu.SemaphoreType.DMA
    vmem = pl.BlockSpec(memory_space=pltpu.VMEM)
    hbm = pl.BlockSpec(memory_space=pltpu.HBM)
    return pl.pallas_call(
        functools.partial(exchange_kernel, nk, nch),
        out_shape=pltpu.VMEM(tokens.shape, BF),
        in_specs=[hbm] * 7,
        out_specs=vmem,
        scratch_shapes=[
            pltpu.VMEM((images, patches, width), BF),
            pltpu.VMEM((n_exp, width), BF),
            pltpu.SMEM((1,), F32),
            pltpu.VMEM((1, hid), BF),
            pltpu.VMEM((n_exp, width), BF),
            pltpu.VMEM((HALVES, 2, cols, ih * patches), BF),
            pltpu.VMEM((width, cols), BF),
            pltpu.VMEM((images * patches, cols), F32),
            pltpu.VMEM((4 * sub, 4 * sub), BF),
            pltpu.VMEM((4 * sub, 4 * sub), BF),
            pltpu.VMEM((2, width, hid), BF),
            pltpu.VMEM((2, hid, width), BF),
            pltpu.VMEM((1, hid), BF),
            pltpu.VMEM((nch, 4 * sub, LN), BF),
            pltpu.VMEM((units, nk, tile, LN), BF),
            pltpu.VMEM((units, nk, tile, LN), BF),
            pltpu.VMEM((units, 2, 5, 2 * sub, LN), BF),
            pltpu.VMEM((HALVES, 2 * nch, 8 * sub, DC), F32),
            pltpu.VMEM((HALVES, 8 * sub, 2 * hid), BF),
            pltpu.VMEM((8 * sub, width), BF),
            pltpu.VMEM((units, 2, 4, 2 * sub, LN), BF),
            pltpu.VMEM((units, 2, 4, 2 * sub, LN), BF),
            pltpu.VMEM((units, nk, tile, LN), BF),
            pltpu.VMEM((HALVES, 2, ih * patches, cols), BF),
            pltpu.VMEM((units, nk, tile, LN), BF),
            dma((images,)),
            dma((6,)),
            dma((3,)),
            dma((3,)),
            dma,
            dma((units, 2)),
            dma,
            dma((units,)),
            dma,
            dma((units, 2)),
            dma,
            dma((units,)),
        ],
        compiler_params=pltpu.CompilerParams(
            collective_id=0, has_side_effects=True, vmem_limit_bytes=58 * 1024 * 1024
        ),
        name="exchange",
    )(tokens, slot_keys.T, logit_scale, up_weight, up_bias, down_weight, down_bias)


def solution(mesh):
    return jax.shard_map(
        body,
        mesh=mesh,
        in_specs=(
            P(("dp", "expert"), None, None),
            P(),
            P(),
            P("expert", None, "dp"),
            P("expert", "dp"),
            P("expert", "dp", None),
            P(),
        ),
        out_specs=P(("dp", "expert"), None, None),
        check_vma=False,
    )
```
